32 devices in a mesh: gx: 2 (over x), gy: 4 (over z), gz: 4 (over y, core).
Axes of the slice: x: 2, y: 2, z: 4, core: 2. Of those that a mesh axis runs over, the one named last changes fastest.
Arguments:
- density: float32 [192, 256, 512], P('gz', 'gx', 'gy'), may hold values from 0.0005 to 0.01
- shear_offsets: int32 [2, 192], P(None, 'gz'), may hold values from 0 to 48, as said below
- shear_fractions: float32 [2, 192], P(None, 'gz'), may hold values from 0 to 1
- flat_field: float32 [256, 512], P(('gx', 'gz'), 'gy'), may hold values from 0.5 to 1.5
Outputs:
- normalized: float32 [256, 512], P(('gx', 'gz'), 'gy')
The draws below stay inside these ranges and needn't reach their ends.
Inputs may be any that keep to these rules, and one draw needn't show every extreme that they name: `shear_offsets`: in each row, the shift never falls from one slice to the next and rises by at most 1; it is 0 or 1 at slice 0 and exactly 48 at the last slice.
All inputs are finite; a program needn't handle non-finite values.
Results may differ from the reference program's by a relative error of at most 0.0003.
Values sent between devices are 32-bit elements; how exact they have to be, the bound alone decides.
A program may use at most 64 MiB of HBM per device.

```python
import math
import jax
import jax.numpy as jnp
from jax import lax

NX = 256
NY = 512
NZ = 192


def draw_shear_offsets(key, part):
    rows_list = []
    for component in range(2):
        shuffled = jax.random.permutation(jax.random.fold_in(key, 11 + component), NZ)
        rising = (shuffled < NZ // 4).astype(jnp.int32)
        rows_list.append(jnp.cumsum(rising).astype(jnp.int32))
    return jnp.stack(rows_list, axis=0)


def steps_of(stream_key, extent, shards, least, high):
    def one(dim, parts):
        draws = jax.random.uniform(jax.random.fold_in(jax.random.fold_in(stream_key, 6), dim), (parts,), jnp.float32, least / len(shards), high / len(shards))
        return jnp.repeat(jnp.exp(draws), extent[dim] // parts).reshape((-1,) + (1,) * (len(extent) - dim - 1))

    level = one(*shards[0])
    for cut in shards[1:]:
        level = level * one(*cut)
    return level


def setup_inputs(seed: int = 0) -> dict:
    keys = jax.random.split(jax.random.key(seed), 5)
    density = jnp.clip(jnp.exp(math.log(0.01) - 2.9957322 * jax.random.uniform(keys[0], (NZ, NX, NY), jnp.float32) ** steps_of(keys[0], (NZ, NX, NY), ((0, 4), (1, 2), (2, 4)), -0.2, 0.2)), 0.0005, 0.01)
    shear_offsets = draw_shear_offsets(jax.random.fold_in(keys[4], 71), 0)
    shear_fractions = jnp.clip(1.0 * jax.random.uniform(keys[2], (2, NZ), jnp.float32) ** steps_of(keys[2], (2, NZ), ((1, 4),), -0.2, 0.2), 0.0, 1.0)
    flat_field = jnp.clip(1.0 + 0.1 * jax.random.normal(keys[3], (NX, NY), jnp.float32), 0.5, 1.5)
    return {"density": density, "shear_offsets": shear_offsets, "shear_fractions": shear_fractions, "flat_field": flat_field}


def splat_slab(screen, slab, start_u, start_v, frac_u, frac_v):
    height, width = slab.shape
    spread = jnp.pad(slab * ((1.0 - frac_u) * (1.0 - frac_v)), ((0, 1), (0, 1)))
    spread = spread + jnp.pad(slab * (frac_u * (1.0 - frac_v)), ((1, 0), (0, 1)))
    spread = spread + jnp.pad(slab * ((1.0 - frac_u) * frac_v), ((0, 1), (1, 0)))
    spread = spread + jnp.pad(slab * (frac_u * frac_v), ((1, 0), (1, 0)))
    window = lax.dynamic_slice(screen, (start_u, start_v), (height + 1, width + 1))
    return lax.dynamic_update_slice(screen, window + spread, (start_u, start_v))


def reference(density, shear_offsets, shear_fractions, flat_field):
    center = NZ // 8
    margin = center + 1
    screen = jnp.zeros((NX + 2 * margin, NY + 2 * margin), jnp.float32)

    def march_slab(carry, inputs):
        slab, offset_pair, frac_pair = inputs
        start_u = (offset_pair[0] - center + margin).astype(jnp.int32)
        start_v = (offset_pair[1] - center + margin).astype(jnp.int32)
        return splat_slab(carry, slab, start_u, start_v, frac_pair[0], frac_pair[1]), None

    screen, unused = lax.scan(march_slab, screen, (density, shear_offsets.T, shear_fractions.T))
    integral = screen[margin:margin + NX, margin:margin + NY]
    detected = flat_field * jnp.exp(-integral)
    return detected / jnp.max(detected)
```

```python
import functools

import jax
import jax.numpy as jnp
from jax import lax
from jax.experimental import pallas as pl
from jax.experimental.pallas import tpu as pltpu
from jax.sharding import PartitionSpec as P

MESH = pl.DeviceIdType.MESH


def plan(tile_rows, tile_cols, slices, nx, ny, nz):
    center = slices * nz // 8
    height = tile_rows // nz
    below = -(-center // height)
    above = -(-(center + 1) // height)
    pad = (max(below, above) * height + center + 8) // 8 * 8
    pad = max(pad, 8)
    packed = 2 * center + 1 <= tile_cols
    return center, height, below, above, pad, packed


def kernel(
    nx, ny, nz, offsets, fracs, flat, density, out,
    volume, staged, landed, total, peak, peaks,
    in_sem, send_sem, recv_sem, peak_send, peak_recv,
):
    slices, tile_rows, tile_cols = density.shape
    center, height, below, above, pad, packed = plan(tile_rows, tile_cols, slices, nx, ny, nz)
    stride = tile_rows + pad
    devices = nx * ny * nz
    ix, iy, iz = lax.axis_index("gx"), lax.axis_index("gy"), lax.axis_index("gz")
    me = (ix * ny + iy) * nz + iz

    def place(index):
        return (index // (ny * nz), (index // nz) % ny, index % nz)

    def fetch(z):
        return pltpu.make_async_copy(
            density.at[z], volume.at[pl.ds(pad + z * stride, tile_rows)], in_sem.at[z]
        )

    @pl.loop(0, slices)
    def _(z):
        fetch(z).start()

    barrier = pltpu.get_barrier_semaphore()

    @pl.loop(1, devices)
    def _(k):
        pl.semaphore_signal(
            barrier, inc=1, device_id=place((me + k) % devices), device_id_type=MESH
        )

    volume[pl.ds(0, pad), :] = jnp.zeros((pad, tile_cols), jnp.float32)

    @pl.loop(0, slices)
    def _(z):
        start = pl.multiple_of(pad + z * stride + tile_rows, 8)
        volume[pl.ds(start, pad), :] = jnp.zeros((pad, tile_cols), jnp.float32)

    @pl.loop(0, slices)
    def _(z):
        fetch(z).wait()
        base = pl.multiple_of(pad + z * stride, 8)
        here = volume[pl.ds(base, tile_rows + 8), :]
        before = volume[pl.ds(base - 1, tile_rows + 8), :]
        mixed = here + fracs[0, z] * (before - here)
        turn = lax.rem(offsets[1, z] - center + tile_cols, tile_cols)
        volume[pl.ds(base, tile_rows + 8), :] = pltpu.roll(mixed, turn, 1)

    pl.semaphore_wait(barrier, devices - 1)

    lane = lax.broadcasted_iota(jnp.int32, (height, tile_cols), 1)
    edges = 1 if packed else 2

    def messages(block):
        step = (block + nz) // nz - 1
        row = block - step * nz
        source = (step + 3) % 3
        found = []
        for side, (shift, tile) in enumerate(((0, 0), (1, 1), (-1, edges))):
            exists = (iy + shift >= 0) & (iy + shift < ny)
            if side == 0:
                exists = (step != 0) | (row != iz)
            copy = pltpu.make_async_remote_copy(
                src_ref=staged.at[block + below, tile],
                dst_ref=landed.at[source, side, iz],
                send_sem=send_sem.at[block + below, side],
                recv_sem=recv_sem.at[source, side, iz],
                device_id=(ix + step, iy + shift, row),
                device_id_type=MESH,
            )
            found.append((exists, copy))
        return found

    def project(block):
        zero = jnp.zeros((height, tile_cols), jnp.float32)
        first = pad + block * height + center

        def add(z, sums):
            whole, late, *parts = sums
            value = volume[pl.ds(first + z * stride - offsets[0, z], height), :]
            moved = value * fracs[1, z]
            turn = offsets[1, z] - center
            right = lane < turn
            left = lane >= tile_cols + turn
            masks = (right | left,) if packed else (right, left)
            grown = [whole + value, late + moved]
            for n, mask in enumerate(masks):
                grown.append(parts[2 * n] + jnp.where(mask, value, 0.0))
                grown.append(parts[2 * n + 1] + jnp.where(mask, moved, 0.0))
            return tuple(grown)

        unroll = next(n for n in (8, 4, 2, 1) if slices % n == 0)

        def several(group, sums):
            for n in range(unroll):
                sums = add(group * unroll + n, sums)
            return sums

        whole, late, *parts = lax.fori_loop(
            0, slices // unroll, several, (zero,) * (2 + 2 * edges)
        )
        for n in range(edges):
            whole = whole - parts[2 * n]
            late = late - parts[2 * n + 1]
        turned = pltpu.roll(late, 1, 1)
        ends = [pltpu.roll(parts[2 * n + 1], 1, 1) for n in range(edges)]
        begin = lane == 0
        staged[block + below, 0] = whole - late + jnp.where(begin, ends[-1], turned)
        staged[block + below, 1] = parts[0] - parts[1] + jnp.where(begin, turned, ends[0])
        if not packed:
            staged[block + below, 2] = parts[2] - parts[3] + jnp.where(begin, 0.0, ends[1])
        for exists, copy in messages(block):
            @pl.when(exists)
            def _():
                copy.start()

    def own(k):
        cores = 2 if nz % 2 == 0 else 1
        chips = nz // cores
        chip, core = iz // cores, iz % cores
        return ((chip + 1 + k // cores) % chips) * cores + (core + 1 + k) % cores

    @pl.when(ix > 0)
    def _():
        @pl.loop(0, below)
        def _(k):
            project(k - below)

    @pl.when(ix < nx - 1)
    def _():
        @pl.loop(0, above)
        def _(k):
            project(nz + k)

    @pl.loop(0, nz)
    def _(k):
        project(own(k))

    total[...] = staged[iz + below, 0]
    for side, beside in ((0, None), (1, iy > 0), (2, iy < ny - 1)):
        for source, within in ((1, (ix > 0) & (iz < above)), (2, (ix < nx - 1) & (iz >= nz - below)), (0, None)):
            def collect(j):
                slot = landed.at[source, side, j]
                pltpu.make_async_remote_copy(
                    src_ref=slot, dst_ref=slot, send_sem=send_sem.at[0, 0],
                    recv_sem=recv_sem.at[source, side, j],
                    device_id=(ix, iy, iz), device_id_type=MESH,
                ).wait_recv()
                value = slot[...]
                if side == 1:
                    value = jnp.where(lane <= center, value, 0.0)
                if side == 2:
                    value = jnp.where(lane >= tile_cols - center, value, 0.0)
                total[...] += value

            def gather():
                @pl.loop(0, nz)
                def _(j):
                    if source == 0 and side == 0:
                        pl.when(j != iz)(lambda: collect(j))
                    else:
                        collect(j)

            cond = [c for c in (beside, within) if c is not None]
            if cond:
                pl.when(functools.reduce(lambda a, b: a & b, cond))(gather)
            else:
                gather()

    detected = flat[...] * jnp.exp(-total[...])
    peak[...] = jnp.max(detected, axis=0, keepdims=True)

    def tell(k):
        return pltpu.make_async_remote_copy(
            src_ref=peak,
            dst_ref=peaks.at[me],
            send_sem=peak_send,
            recv_sem=peak_recv,
            device_id=place((me + k) % devices),
            device_id_type=MESH,
        )

    @pl.loop(1, devices)
    def _(k):
        tell(k).start()

    peaks[me] = peak[...]
    others = peaks.at[pl.ds(0, devices - 1)]
    pltpu.make_async_copy(others, others, peak_recv).wait()
    out[...] = detected / jnp.max(peaks[...])
    pltpu.make_async_copy(others, others, peak_send).wait()

    def drain(block):
        for exists, copy in messages(block):
            @pl.when(exists)
            def _():
                copy.wait_send()

    @pl.when(ix > 0)
    def _():
        @pl.loop(0, below)
        def _(k):
            drain(k - below)

    @pl.when(ix < nx - 1)
    def _():
        @pl.loop(0, above)
        def _(k):
            drain(nz + k)

    @pl.loop(0, nz)
    def _(k):
        drain(k)


def solution(mesh):
    nx, ny, nz = mesh.shape["gx"], mesh.shape["gy"], mesh.shape["gz"]

    def shards(density, shear_offsets, shear_fractions, flat_field):
        slices, tile_rows, tile_cols = density.shape
        center, height, below, above, pad, packed = plan(tile_rows, tile_cols, slices, nx, ny, nz)
        blocks = below + nz + above
        devices = nx * ny * nz
        block = (height, tile_cols)
        return pl.pallas_call(
            functools.partial(kernel, nx, ny, nz),
            out_shape=jax.ShapeDtypeStruct(block, jnp.float32),
            in_specs=[
                pl.BlockSpec(memory_space=pltpu.SMEM),
                pl.BlockSpec(memory_space=pltpu.SMEM),
                pl.BlockSpec(memory_space=pltpu.VMEM),
                pl.BlockSpec(memory_space=pl.ANY),
            ],
            out_specs=pl.BlockSpec(memory_space=pltpu.VMEM),
            scratch_shapes=[
                pltpu.VMEM((pad + slices * (tile_rows + pad), tile_cols), jnp.float32),
                pltpu.VMEM((blocks, 2 if packed else 3) + block, jnp.float32),
                pltpu.VMEM((3, 3, nz) + block, jnp.float32),
                pltpu.VMEM(block, jnp.float32),
                pltpu.VMEM((1, tile_cols), jnp.float32),
                pltpu.VMEM((devices, 1, tile_cols), jnp.float32),
                pltpu.SemaphoreType.DMA((slices,)),
                pltpu.SemaphoreType.DMA((blocks, 3)),
                pltpu.SemaphoreType.DMA((3, 3, nz)),
                pltpu.SemaphoreType.DMA,
                pltpu.SemaphoreType.DMA,
            ],
            compiler_params=pltpu.CompilerParams(collective_id=0, has_side_effects=True),
        )(shear_offsets, shear_fractions, flat_field, density)

    in_specs = (P("gz", "gx", "gy"), P(None, "gz"), P(None, "gz"), P(("gx", "gz"), "gy"))
    out_specs = P(("gx", "gz"), "gy")
    return jax.shard_map(shards, mesh=mesh, in_specs=in_specs, out_specs=out_specs, check_vma=False)
```

```python
import functools

import jax
import jax.numpy as jnp
from jax import lax
from jax.experimental import pallas as pl
from jax.experimental.pallas import tpu as pltpu
from jax.sharding import PartitionSpec as P

MESH = pl.DeviceIdType.MESH


def plan(tile_rows, tile_cols, slices, nx, ny, nz):
    center = slices * nz // 8
    height = tile_rows // nz
    below = -(-center // height)
    above = -(-(center + 1) // height)
    pad = (max(below, above) * height + center + 8) // 8 * 8
    pad = max(pad, 8)
    packed = 2 * center + 1 <= tile_cols
    return center, height, below, above, pad, packed


def kernel(
    nx, ny, nz, offsets_in, fracs_in, flat_in, density, out,
    offsets, fracs, flat, arrived, volume, staged, landed, total, peak, peaks,
    small_sem, in_sem, send_sem, recv_sem, peak_send, peak_recv,
):
    slices, tile_rows, tile_cols = density.shape
    center, height, below, above, pad, packed = plan(tile_rows, tile_cols, slices, nx, ny, nz)
    stride = tile_rows + pad
    devices = nx * ny * nz
    ix, iy, iz = lax.axis_index("gx"), lax.axis_index("gy"), lax.axis_index("gz")
    me = (ix * ny + iy) * nz + iz

    def place(index):
        return (index // (ny * nz), (index // nz) % ny, index % nz)

    group = next(n for n in (8, 4, 2, 1) if slices % n == 0)
    small = [
        pltpu.make_async_copy(source, target, small_sem.at[n])
        for n, (source, target) in enumerate(
            ((offsets_in, offsets), (fracs_in, fracs), (flat_in, flat))
        )
    ]
    for copy in small:
        copy.start()

    def fetch(n):
        first = n * group
        return pltpu.make_async_copy(
            density.at[pl.ds(first, group)],
            arrived.at[pl.ds(first, group), pl.ds(8, tile_rows)],
            in_sem.at[n],
        )

    @pl.loop(0, slices // group)
    def _(n):
        fetch(n).start()

    barrier = pltpu.get_barrier_semaphore()

    @pl.loop(1, devices)
    def _(k):
        pl.semaphore_signal(
            barrier, inc=1, device_id=place((me + k) % devices), device_id_type=MESH
        )

    volume[pl.ds(0, pad), :] = jnp.zeros((pad, tile_cols), jnp.float32)

    @pl.loop(0, slices)
    def _(z):
        start = pl.multiple_of(pad + z * stride + tile_rows, 8)
        volume[pl.ds(start, pad), :] = jnp.zeros((pad, tile_cols), jnp.float32)
        arrived[z, pl.ds(0, 8), :] = jnp.zeros((8, tile_cols), jnp.float32)
        arrived[z, pl.ds(8 + tile_rows, 8), :] = jnp.zeros((8, tile_cols), jnp.float32)

    for copy in small:
        copy.wait()

    @pl.loop(0, slices // group)
    def _(n):
        fetch(n).wait()
        for k in range(group):
            z = n * group + k
            here = arrived[z, pl.ds(8, tile_rows + 8), :]
            before = arrived[z, pl.ds(7, tile_rows + 8), :]
            mixed = here + fracs[0, z] * (before - here)
            turn = lax.rem(offsets[1, z] - center + tile_cols, tile_cols)
            base = pl.multiple_of(pad + z * stride, 8)
            volume[pl.ds(base, tile_rows + 8), :] = pltpu.roll(mixed, turn, 1)

    pl.semaphore_wait(barrier, devices - 1)

    lane = lax.broadcasted_iota(jnp.int32, (height, tile_cols), 1)
    edges = 1 if packed else 2

    def messages(block):
        step = (block + nz) // nz - 1
        row = block - step * nz
        source = (step + 3) % 3
        found = []
        for side, (shift, tile) in enumerate(((0, 0), (1, 1), (-1, edges))):
            exists = (iy + shift >= 0) & (iy + shift < ny)
            if side == 0:
                exists = (step != 0) | (row != iz)
            copy = pltpu.make_async_remote_copy(
                src_ref=staged.at[block + below, tile],
                dst_ref=landed.at[source, side, iz],
                send_sem=send_sem.at[block + below, side],
                recv_sem=recv_sem.at[source, side, iz],
                device_id=(ix + step, iy + shift, row),
                device_id_type=MESH,
            )
            found.append((exists, copy))
        return found

    def project(block):
        zero = jnp.zeros((height, tile_cols), jnp.float32)
        first = pad + block * height + center

        def add(z, sums):
            whole, late, *parts = sums
            value = volume[pl.ds(first + z * stride - offsets[0, z], height), :]
            moved = value * fracs[1, z]
            turn = offsets[1, z] - center
            right = lane < turn
            left = lane >= tile_cols + turn
            masks = (right | left,) if packed else (right, left)
            grown = [whole + value, late + moved]
            for n, mask in enumerate(masks):
                grown.append(parts[2 * n] + jnp.where(mask, value, 0.0))
                grown.append(parts[2 * n + 1] + jnp.where(mask, moved, 0.0))
            return tuple(grown)

        unroll = next(n for n in (8, 4, 2, 1) if slices % n == 0)

        def several(group, sums):
            for n in range(unroll):
                sums = add(group * unroll + n, sums)
            return sums

        whole, late, *parts = lax.fori_loop(
            0, slices // unroll, several, (zero,) * (2 + 2 * edges)
        )
        for n in range(edges):
            whole = whole - parts[2 * n]
            late = late - parts[2 * n + 1]
        turned = pltpu.roll(late, 1, 1)
        ends = [pltpu.roll(parts[2 * n + 1], 1, 1) for n in range(edges)]
        begin = lane == 0
        staged[block + below, 0] = whole - late + jnp.where(begin, ends[-1], turned)
        staged[block + below, 1] = parts[0] - parts[1] + jnp.where(begin, turned, ends[0])
        if not packed:
            staged[block + below, 2] = parts[2] - parts[3] + jnp.where(begin, 0.0, ends[1])
        for exists, copy in messages(block):
            @pl.when(exists)
            def _():
                copy.start()

    def own(k):
        cores = 2 if nz % 2 == 0 else 1
        chips = nz // cores
        chip, core = iz // cores, iz % cores
        return ((chip + 1 + k // cores) % chips) * cores + (core + 1 + k) % cores

    @pl.when(ix > 0)
    def _():
        @pl.loop(0, below)
        def _(k):
            project(k - below)

    @pl.when(ix < nx - 1)
    def _():
        @pl.loop(0, above)
        def _(k):
            project(nz + k)

    @pl.loop(0, nz)
    def _(k):
        project(own(k))

    total[...] = staged[iz + below, 0]
    for side, beside in ((0, None), (1, iy > 0), (2, iy < ny - 1)):
        for source, within in ((1, (ix > 0) & (iz < above)), (2, (ix < nx - 1) & (iz >= nz - below)), (0, None)):
            def collect(j):
                slot = landed.at[source, side, j]
                pltpu.make_async_remote_copy(
                    src_ref=slot, dst_ref=slot, send_sem=send_sem.at[0, 0],
                    recv_sem=recv_sem.at[source, side, j],
                    device_id=(ix, iy, iz), device_id_type=MESH,
                ).wait_recv()
                value = slot[...]
                if side == 1:
                    value = jnp.where(lane <= center, value, 0.0)
                if side == 2:
                    value = jnp.where(lane >= tile_cols - center, value, 0.0)
                total[...] += value

            def gather():
                @pl.loop(0, nz)
                def _(j):
                    if source == 0 and side == 0:
                        pl.when(j != iz)(lambda: collect(j))
                    else:
                        collect(j)

            cond = [c for c in (beside, within) if c is not None]
            if cond:
                pl.when(functools.reduce(lambda a, b: a & b, cond))(gather)
            else:
                gather()

    detected = flat[...] * jnp.exp(-total[...])
    peak[...] = jnp.max(detected, axis=0, keepdims=True)

    def tell(k):
        return pltpu.make_async_remote_copy(
            src_ref=peak,
            dst_ref=peaks.at[me],
            send_sem=peak_send,
            recv_sem=peak_recv,
            device_id=place((me + k) % devices),
            device_id_type=MESH,
        )

    @pl.loop(1, devices)
    def _(k):
        tell(k).start()

    peaks[me] = peak[...]
    others = peaks.at[pl.ds(0, devices - 1)]
    pltpu.make_async_copy(others, others, peak_recv).wait()
    out[...] = detected / jnp.max(peaks[...])
    pltpu.make_async_copy(others, others, peak_send).wait()

    def drain(block):
        for exists, copy in messages(block):
            @pl.when(exists)
            def _():
                copy.wait_send()

    @pl.when(ix > 0)
    def _():
        @pl.loop(0, below)
        def _(k):
            drain(k - below)

    @pl.when(ix < nx - 1)
    def _():
        @pl.loop(0, above)
        def _(k):
            drain(nz + k)

    @pl.loop(0, nz)
    def _(k):
        drain(k)


def solution(mesh):
    nx, ny, nz = mesh.shape["gx"], mesh.shape["gy"], mesh.shape["gz"]

    def shards(density, shear_offsets, shear_fractions, flat_field):
        slices, tile_rows, tile_cols = density.shape
        center, height, below, above, pad, packed = plan(tile_rows, tile_cols, slices, nx, ny, nz)
        blocks = below + nz + above
        devices = nx * ny * nz
        block = (height, tile_cols)
        return pl.pallas_call(
            functools.partial(kernel, nx, ny, nz),
            out_shape=jax.ShapeDtypeStruct(block, jnp.float32),
            in_specs=[
                pl.BlockSpec(memory_space=pl.ANY),
            ] * 4,
            out_specs=pl.BlockSpec(memory_space=pltpu.VMEM),
            scratch_shapes=[
                pltpu.SMEM(shear_offsets.shape, jnp.int32),
                pltpu.SMEM(shear_fractions.shape, jnp.float32),
                pltpu.VMEM(block, jnp.float32),
                pltpu.VMEM((slices, tile_rows + 16, tile_cols), jnp.float32),
                pltpu.VMEM((pad + slices * (tile_rows + pad), tile_cols), jnp.float32),
                pltpu.VMEM((blocks, 2 if packed else 3) + block, jnp.float32),
                pltpu.VMEM((3, 3, nz) + block, jnp.float32),
                pltpu.VMEM(block, jnp.float32),
                pltpu.VMEM((1, tile_cols), jnp.float32),
                pltpu.VMEM((devices, 1, tile_cols), jnp.float32),
                pltpu.SemaphoreType.DMA((3,)),
                pltpu.SemaphoreType.DMA((slices,)),
                pltpu.SemaphoreType.DMA((blocks, 3)),
                pltpu.SemaphoreType.DMA((3, 3, nz)),
                pltpu.SemaphoreType.DMA,
                pltpu.SemaphoreType.DMA,
            ],
            compiler_params=pltpu.CompilerParams(collective_id=0, has_side_effects=True),
        )(shear_offsets, shear_fractions, flat_field, density)

    in_specs = (P("gz", "gx", "gy"), P(None, "gz"), P(None, "gz"), P(("gx", "gz"), "gy"))
    out_specs = P(("gx", "gz"), "gy")
    return jax.shard_map(shards, mesh=mesh, in_specs=in_specs, out_specs=out_specs, check_vma=False)
```

```python
import functools

import jax
import jax.numpy as jnp
from jax import lax
from jax.experimental import pallas as pl
from jax.experimental.pallas import tpu as pltpu
from jax.sharding import PartitionSpec as P

MESH = pl.DeviceIdType.MESH


def plan(tile_rows, tile_cols, slices, nx, ny, nz):
    center = slices * nz // 8
    height = tile_rows // nz
    below = -(-center // height)
    above = -(-(center + 1) // height)
    pad = (max(below, above) * height + center + 8) // 8 * 8
    pad = max(pad, 8)
    packed = 2 * center + 1 <= tile_cols
    return center, height, below, above, pad, packed


def kernel(
    nx, ny, nz, offsets_in, fracs_in, flat_in, density, out,
    offsets, fracs, flat, arrived, volume, staged, landed, total, peak, peaks,
    small_sem, in_sem, send_sem, recv_sem, peak_send, peak_recv,
):
    slices, tile_rows, tile_cols = density.shape
    center, height, below, above, pad, packed = plan(tile_rows, tile_cols, slices, nx, ny, nz)
    stride = tile_rows + pad
    devices = nx * ny * nz
    ix, iy, iz = lax.axis_index("gx"), lax.axis_index("gy"), lax.axis_index("gz")
    me = (ix * ny + iy) * nz + iz

    def place(index):
        return (index // (ny * nz), (index // nz) % ny, index % nz)

    group = next(n for n in (8, 4, 2, 1) if slices % n == 0)
    small = [
        pltpu.make_async_copy(source, target, small_sem.at[n])
        for n, (source, target) in enumerate(
            ((offsets_in, offsets), (fracs_in, fracs), (flat_in, flat))
        )
    ]
    for copy in small:
        copy.start()

    def fetch(n):
        first = n * group
        return pltpu.make_async_copy(
            density.at[pl.ds(first, group)],
            arrived.at[pl.ds(first, group), pl.ds(8, tile_rows)],
            in_sem.at[n],
        )

    @pl.loop(0, slices // group)
    def _(n):
        fetch(n).start()

    barrier = pltpu.get_barrier_semaphore()

    @pl.loop(1, devices, unroll=devices <= 32)
    def _(k):
        pl.semaphore_signal(
            barrier, inc=1, device_id=place((me + k) % devices), device_id_type=MESH
        )

    volume[pl.ds(0, pad), :] = jnp.zeros((pad, tile_cols), jnp.float32)

    @pl.loop(0, slices)
    def _(z):
        start = pl.multiple_of(pad + z * stride + tile_rows, 8)
        volume[pl.ds(start, pad), :] = jnp.zeros((pad, tile_cols), jnp.float32)
        arrived[z, pl.ds(0, 8), :] = jnp.zeros((8, tile_cols), jnp.float32)
        arrived[z, pl.ds(8 + tile_rows, 8), :] = jnp.zeros((8, tile_cols), jnp.float32)

    for copy in small:
        copy.wait()

    @pl.loop(0, slices // group)
    def _(n):
        fetch(n).wait()
        for k in range(group):
            z = n * group + k
            here = arrived[z, pl.ds(8, tile_rows + 8), :]
            before = arrived[z, pl.ds(7, tile_rows + 8), :]
            mixed = here + fracs[0, z] * (before - here)
            turn = lax.rem(offsets[1, z] - center + tile_cols, tile_cols)
            base = pl.multiple_of(pad + z * stride, 8)
            volume[pl.ds(base, tile_rows + 8), :] = pltpu.roll(mixed, turn, 1)

    lane = lax.broadcasted_iota(jnp.int32, (height, tile_cols), 1)
    edges = 1 if packed else 2

    def messages(block):
        step = (block + nz) // nz - 1
        row = block - step * nz
        source = (step + 3) % 3
        found = []
        for side, (shift, tile) in enumerate(((0, 0), (1, 1), (-1, edges))):
            exists = (iy + shift >= 0) & (iy + shift < ny)
            if side == 0:
                exists = (step != 0) | (row != iz)
            copy = pltpu.make_async_remote_copy(
                src_ref=staged.at[block + below, tile],
                dst_ref=landed.at[source, side, iz],
                send_sem=send_sem.at[block + below, side],
                recv_sem=recv_sem.at[source, side, iz],
                device_id=(ix + step, iy + shift, row),
                device_id_type=MESH,
            )
            found.append((exists, copy))
        return found

    def project(block):
        zero = jnp.zeros((height, tile_cols), jnp.float32)
        first = pad + block * height + center

        def add(z, sums):
            whole, late, *parts = sums
            value = volume[pl.ds(first + z * stride - offsets[0, z], height), :]
            moved = value * fracs[1, z]
            turn = offsets[1, z] - center
            right = lane < turn
            left = lane >= tile_cols + turn
            masks = (right | left,) if packed else (right, left)
            grown = [whole + value, late + moved]
            for n, mask in enumerate(masks):
                grown.append(parts[2 * n] + jnp.where(mask, value, 0.0))
                grown.append(parts[2 * n + 1] + jnp.where(mask, moved, 0.0))
            return tuple(grown)

        unroll = next(n for n in (8, 4, 2, 1) if slices % n == 0)

        def several(group, sums):
            for n in range(unroll):
                sums = add(group * unroll + n, sums)
            return sums

        whole, late, *parts = lax.fori_loop(
            0, slices // unroll, several, (zero,) * (2 + 2 * edges)
        )
        for n in range(edges):
            whole = whole - parts[2 * n]
            late = late - parts[2 * n + 1]
        turned = pltpu.roll(late, 1, 1)
        ends = [pltpu.roll(parts[2 * n + 1], 1, 1) for n in range(edges)]
        begin = lane == 0
        staged[block + below, 0] = whole - late + jnp.where(begin, ends[-1], turned)
        staged[block + below, 1] = parts[0] - parts[1] + jnp.where(begin, turned, ends[0])
        if not packed:
            staged[block + below, 2] = parts[2] - parts[3] + jnp.where(begin, 0.0, ends[1])
    def send(block):
        for exists, copy in messages(block):
            pl.when(exists)(copy.start)

    def own(k):
        cores = 2 if nz % 2 == 0 else 1
        chips = nz // cores
        chip, core = iz // cores, iz % cores
        return ((chip + 1 + k // cores) % chips) * cores + (core + 1 + k) % cores

    def border(act):
        @pl.when(ix > 0)
        def _():
            pl.loop(0, below)(lambda k: act(k - below))

        @pl.when(ix < nx - 1)
        def _():
            pl.loop(0, above)(lambda k: act(nz + k))

    early = nz // 2
    border(project)
    if early:
        pl.loop(0, early)(lambda k: project(own(k)))
    pl.semaphore_wait(barrier, devices - 1)
    border(send)
    if early:
        pl.loop(0, early)(lambda k: send(own(k)))

    if early < nz:
        @pl.loop(early, nz)
        def _(k):
            project(own(k))
            send(own(k))

    total[...] = staged[iz + below, 0]
    for side, beside in ((0, None), (1, iy > 0), (2, iy < ny - 1)):
        for source, within in ((1, (ix > 0) & (iz < above)), (2, (ix < nx - 1) & (iz >= nz - below)), (0, None)):
            def collect(j):
                slot = landed.at[source, side, j]
                pltpu.make_async_remote_copy(
                    src_ref=slot, dst_ref=slot, send_sem=send_sem.at[0, 0],
                    recv_sem=recv_sem.at[source, side, j],
                    device_id=(ix, iy, iz), device_id_type=MESH,
                ).wait_recv()
                value = slot[...]
                if side == 1:
                    value = jnp.where(lane <= center, value, 0.0)
                if side == 2:
                    value = jnp.where(lane >= tile_cols - center, value, 0.0)
                total[...] += value

            def gather():
                @pl.loop(0, nz, unroll=nz <= 4)
                def _(j):
                    if source == 0 and side == 0:
                        pl.when(j != iz)(lambda: collect(j))
                    else:
                        collect(j)

            cond = [c for c in (beside, within) if c is not None]
            if cond:
                pl.when(functools.reduce(lambda a, b: a & b, cond))(gather)
            else:
                gather()

    detected = flat[...] * jnp.exp(-total[...])
    peak[...] = jnp.max(detected, axis=0, keepdims=True)

    def tell(k):
        return pltpu.make_async_remote_copy(
            src_ref=peak,
            dst_ref=peaks.at[me],
            send_sem=peak_send,
            recv_sem=peak_recv,
            device_id=place((me + k) % devices),
            device_id_type=MESH,
        )

    far = devices // 2

    @pl.loop(0, devices - far, unroll=devices <= 32)
    def _(k):
        tell(far + k).start()

    if far > 1:
        @pl.loop(1, far, unroll=devices <= 32)
        def _(k):
            tell(k).start()

    peaks[me] = peak[...]
    others = peaks.at[pl.ds(0, devices - 1)]
    pltpu.make_async_copy(others, others, peak_recv).wait()
    out[...] = detected / jnp.max(peaks[...])
    pltpu.make_async_copy(others, others, peak_send).wait()

    def drain(block):
        for exists, copy in messages(block):
            pl.when(exists)(copy.wait_send)

    border(drain)
    pl.loop(0, nz)(drain)


def solution(mesh):
    nx, ny, nz = mesh.shape["gx"], mesh.shape["gy"], mesh.shape["gz"]

    def shards(density, shear_offsets, shear_fractions, flat_field):
        slices, tile_rows, tile_cols = density.shape
        center, height, below, above, pad, packed = plan(tile_rows, tile_cols, slices, nx, ny, nz)
        blocks = below + nz + above
        devices = nx * ny * nz
        block = (height, tile_cols)
        return pl.pallas_call(
            functools.partial(kernel, nx, ny, nz),
            out_shape=jax.ShapeDtypeStruct(block, jnp.float32),
            in_specs=[
                pl.BlockSpec(memory_space=pl.ANY),
            ] * 4,
            out_specs=pl.BlockSpec(memory_space=pltpu.VMEM),
            scratch_shapes=[
                pltpu.SMEM(shear_offsets.shape, jnp.int32),
                pltpu.SMEM(shear_fractions.shape, jnp.float32),
                pltpu.VMEM(block, jnp.float32),
                pltpu.VMEM((slices, tile_rows + 16, tile_cols), jnp.float32),
                pltpu.VMEM((pad + slices * (tile_rows + pad), tile_cols), jnp.float32),
                pltpu.VMEM((blocks, 2 if packed else 3) + block, jnp.float32),
                pltpu.VMEM((3, 3, nz) + block, jnp.float32),
                pltpu.VMEM(block, jnp.float32),
                pltpu.VMEM((1, tile_cols), jnp.float32),
                pltpu.VMEM((devices, 1, tile_cols), jnp.float32),
                pltpu.SemaphoreType.DMA((3,)),
                pltpu.SemaphoreType.DMA((slices,)),
                pltpu.SemaphoreType.DMA((blocks, 3)),
                pltpu.SemaphoreType.DMA((3, 3, nz)),
                pltpu.SemaphoreType.DMA,
                pltpu.SemaphoreType.DMA,
            ],
            compiler_params=pltpu.CompilerParams(collective_id=0, has_side_effects=True),
        )(shear_offsets, shear_fractions, flat_field, density)

    in_specs = (P("gz", "gx", "gy"), P(None, "gz"), P(None, "gz"), P(("gx", "gz"), "gy"))
    out_specs = P(("gx", "gz"), "gy")
    return jax.shard_map(shards, mesh=mesh, in_specs=in_specs, out_specs=out_specs, check_vma=False)
```

```python
import functools

import jax
import jax.numpy as jnp
from jax import lax
from jax.experimental import pallas as pl
from jax.experimental.pallas import tpu as pltpu
from jax.sharding import PartitionSpec as P

MESH = pl.DeviceIdType.MESH


def plan(tile_rows, tile_cols, slices, nx, ny, nz):
    center = slices * nz // 8
    height = tile_rows // nz
    below = -(-center // height)
    above = -(-(center + 1) // height)
    pad = (max(below, above) * height + center + 8) // 8 * 8
    pad = max(pad, 8)
    packed = 2 * center + 1 <= tile_cols
    return center, height, below, above, pad, packed


def kernel(
    nx, ny, nz, offsets_in, fracs_in, flat_in, density, out,
    offsets, fracs, flat, arrived, volume, staged, landed, total, peak, peaks,
    small_sem, in_sem, send_sem, recv_sem, peak_send, peak_recv,
):
    slices, tile_rows, tile_cols = density.shape
    center, height, below, above, pad, packed = plan(tile_rows, tile_cols, slices, nx, ny, nz)
    stride = tile_rows + pad
    devices = nx * ny * nz
    ix, iy, iz = lax.axis_index("gx"), lax.axis_index("gy"), lax.axis_index("gz")
    me = (ix * ny + iy) * nz + iz

    def place(index):
        return (index // (ny * nz), (index // nz) % ny, index % nz)

    group = next(n for n in (8, 4, 2, 1) if slices % n == 0)
    small = [
        pltpu.make_async_copy(source, target, small_sem.at[n])
        for n, (source, target) in enumerate(
            ((offsets_in, offsets), (fracs_in, fracs), (flat_in, flat))
        )
    ]
    for copy in small:
        copy.start()

    def fetch(n):
        first = n * group
        return pltpu.make_async_copy(
            density.at[pl.ds(first, group)],
            arrived.at[pl.ds(first, group), pl.ds(8, tile_rows)],
            in_sem.at[n],
        )

    @pl.loop(0, slices // group)
    def _(n):
        fetch(n).start()

    barrier = pltpu.get_barrier_semaphore()

    @pl.loop(1, devices, unroll=devices <= 32)
    def _(k):
        pl.semaphore_signal(
            barrier, inc=1, device_id=place((me + k) % devices), device_id_type=MESH
        )

    volume[pl.ds(0, pad), :] = jnp.zeros((pad, tile_cols), jnp.float32)

    @pl.loop(0, slices)
    def _(z):
        start = pl.multiple_of(pad + z * stride + tile_rows, 8)
        volume[pl.ds(start, pad), :] = jnp.zeros((pad, tile_cols), jnp.float32)
        arrived[z, pl.ds(0, 8), :] = jnp.zeros((8, tile_cols), jnp.float32)
        arrived[z, pl.ds(8 + tile_rows, 8), :] = jnp.zeros((8, tile_cols), jnp.float32)

    for copy in small:
        copy.wait()

    @pl.loop(0, slices // group)
    def _(n):
        fetch(n).wait()
        for k in range(group):
            z = n * group + k
            here = arrived[z, pl.ds(8, tile_rows + 8), :]
            before = arrived[z, pl.ds(7, tile_rows + 8), :]
            mixed = here + fracs[0, z] * (before - here)
            turn = lax.rem(offsets[1, z] - center + tile_cols, tile_cols)
            base = pl.multiple_of(pad + z * stride, 8)
            volume[pl.ds(base, tile_rows + 8), :] = pltpu.roll(mixed, turn, 1)

    lane = lax.broadcasted_iota(jnp.int32, (height, tile_cols), 1)
    edges = 1 if packed else 2

    def messages(block):
        step = (block + nz) // nz - 1
        row = block - step * nz
        source = (step + 3) % 3
        found = []
        for side, (shift, tile) in enumerate(((0, 0), (1, 1), (-1, edges))):
            exists = (iy + shift >= 0) & (iy + shift < ny)
            if side == 0:
                exists = (step != 0) | (row != iz)
            copy = pltpu.make_async_remote_copy(
                src_ref=staged.at[block + below, tile],
                dst_ref=landed.at[source, side, iz],
                send_sem=send_sem.at[block + below, side],
                recv_sem=recv_sem.at[source, side, iz],
                device_id=(ix + step, iy + shift, row),
                device_id_type=MESH,
            )
            found.append((exists, copy))
        return found

    def project(block):
        zero = jnp.zeros((height, tile_cols), jnp.float32)
        first = pad + block * height + center

        def add(z, sums):
            whole, late, *parts = sums
            value = volume[pl.ds(first + z * stride - offsets[0, z], height), :]
            moved = value * fracs[1, z]
            turn = offsets[1, z] - center
            right = lane < turn
            left = lane >= tile_cols + turn
            masks = (right | left,) if packed else (right, left)
            grown = [whole + value, late + moved]
            for n, mask in enumerate(masks):
                grown.append(parts[2 * n] + jnp.where(mask, value, 0.0))
                grown.append(parts[2 * n + 1] + jnp.where(mask, moved, 0.0))
            return tuple(grown)

        unroll = next(n for n in (16, 8, 4, 2, 1) if slices % n == 0)

        def several(group, sums):
            for n in range(unroll):
                sums = add(group * unroll + n, sums)
            return sums

        whole, late, *parts = lax.fori_loop(
            0, slices // unroll, several, (zero,) * (2 + 2 * edges)
        )
        for n in range(edges):
            whole = whole - parts[2 * n]
            late = late - parts[2 * n + 1]
        turned = pltpu.roll(late, 1, 1)
        ends = [pltpu.roll(parts[2 * n + 1], 1, 1) for n in range(edges)]
        begin = lane == 0
        staged[block + below, 0] = whole - late + jnp.where(begin, ends[-1], turned)
        staged[block + below, 1] = parts[0] - parts[1] + jnp.where(begin, turned, ends[0])
        if not packed:
            staged[block + below, 2] = parts[2] - parts[3] + jnp.where(begin, 0.0, ends[1])
    def send(block):
        for exists, copy in messages(block):
            pl.when(exists)(copy.start)

    def own(k):
        cores = 2 if nz % 2 == 0 else 1
        chips = nz // cores
        chip, core = iz // cores, iz % cores
        return ((chip + 1 + k // cores) % chips) * cores + (core + 1 + k) % cores

    def border(act):
        @pl.when(ix > 0)
        def _():
            pl.loop(0, below)(lambda k: act(k - below))

        @pl.when(ix < nx - 1)
        def _():
            pl.loop(0, above)(lambda k: act(nz + k))

    early = nz // 2
    border(project)
    if early:
        pl.loop(0, early)(lambda k: project(own(k)))
    pl.semaphore_wait(barrier, devices - 1)
    border(send)
    if early:
        pl.loop(0, early)(lambda k: send(own(k)))

    if early < nz:
        @pl.loop(early, nz)
        def _(k):
            project(own(k))
            send(own(k))

    total[...] = staged[iz + below, 0]
    for side, beside in ((0, None), (1, iy > 0), (2, iy < ny - 1)):
        for source, within in ((1, (ix > 0) & (iz < above)), (2, (ix < nx - 1) & (iz >= nz - below)), (0, None)):
            def collect(j):
                slot = landed.at[source, side, j]
                pltpu.make_async_remote_copy(
                    src_ref=slot, dst_ref=slot, send_sem=send_sem.at[0, 0],
                    recv_sem=recv_sem.at[source, side, j],
                    device_id=(ix, iy, iz), device_id_type=MESH,
                ).wait_recv()
                value = slot[...]
                if side == 1:
                    value = jnp.where(lane <= center, value, 0.0)
                if side == 2:
                    value = jnp.where(lane >= tile_cols - center, value, 0.0)
                total[...] += value

            def gather():
                @pl.loop(0, nz, unroll=nz <= 4)
                def _(j):
                    if source == 0 and side == 0:
                        pl.when(j != iz)(lambda: collect(j))
                    else:
                        collect(j)

            cond = [c for c in (beside, within) if c is not None]
            if cond:
                pl.when(functools.reduce(lambda a, b: a & b, cond))(gather)
            else:
                gather()

    detected = flat[...] * jnp.exp(-total[...])
    peak[...] = jnp.max(detected, axis=0, keepdims=True)

    def tell(k):
        return pltpu.make_async_remote_copy(
            src_ref=peak,
            dst_ref=peaks.at[me],
            send_sem=peak_send,
            recv_sem=peak_recv,
            device_id=place((me + k) % devices),
            device_id_type=MESH,
        )

    far = devices // 2

    @pl.loop(0, devices - far, unroll=devices <= 32)
    def _(k):
        tell(far + k).start()

    if far > 1:
        @pl.loop(1, far, unroll=devices <= 32)
        def _(k):
            tell(k).start()

    peaks[me] = peak[...]
    others = peaks.at[pl.ds(0, devices - 1)]
    pltpu.make_async_copy(others, others, peak_recv).wait()
    out[...] = detected / jnp.max(peaks[...])
    pltpu.make_async_copy(others, others, peak_send).wait()

    def drain(block):
        for exists, copy in messages(block):
            pl.when(exists)(copy.wait_send)

    border(drain)
    pl.loop(0, nz)(drain)


def solution(mesh):
    nx, ny, nz = mesh.shape["gx"], mesh.shape["gy"], mesh.shape["gz"]

    def shards(density, shear_offsets, shear_fractions, flat_field):
        slices, tile_rows, tile_cols = density.shape
        center, height, below, above, pad, packed = plan(tile_rows, tile_cols, slices, nx, ny, nz)
        blocks = below + nz + above
        devices = nx * ny * nz
        block = (height, tile_cols)
        return pl.pallas_call(
            functools.partial(kernel, nx, ny, nz),
            out_shape=jax.ShapeDtypeStruct(block, jnp.float32),
            in_specs=[
                pl.BlockSpec(memory_space=pl.ANY),
            ] * 4,
            out_specs=pl.BlockSpec(memory_space=pltpu.VMEM),
            scratch_shapes=[
                pltpu.SMEM(shear_offsets.shape, jnp.int32),
                pltpu.SMEM(shear_fractions.shape, jnp.float32),
                pltpu.VMEM(block, jnp.float32),
                pltpu.VMEM((slices, tile_rows + 16, tile_cols), jnp.float32),
                pltpu.VMEM((pad + slices * (tile_rows + pad), tile_cols), jnp.float32),
                pltpu.VMEM((blocks, 2 if packed else 3) + block, jnp.float32),
                pltpu.VMEM((3, 3, nz) + block, jnp.float32),
                pltpu.VMEM(block, jnp.float32),
                pltpu.VMEM((1, tile_cols), jnp.float32),
                pltpu.VMEM((devices, 1, tile_cols), jnp.float32),
                pltpu.SemaphoreType.DMA((3,)),
                pltpu.SemaphoreType.DMA((slices,)),
                pltpu.SemaphoreType.DMA((blocks, 3)),
                pltpu.SemaphoreType.DMA((3, 3, nz)),
                pltpu.SemaphoreType.DMA,
                pltpu.SemaphoreType.DMA,
            ],
            compiler_params=pltpu.CompilerParams(collective_id=0, has_side_effects=True),
        )(shear_offsets, shear_fractions, flat_field, density)

    in_specs = (P("gz", "gx", "gy"), P(None, "gz"), P(None, "gz"), P(("gx", "gz"), "gy"))
    out_specs = P(("gx", "gz"), "gy")
    return jax.shard_map(shards, mesh=mesh, in_specs=in_specs, out_specs=out_specs, check_vma=False)
```
